32 devices in a mesh: groups: 2 (over x), chol: 16 (over z, y, core).
Axes of the slice: x: 2, y: 2, z: 4, core: 2. Of those that a mesh axis runs over, the one named last changes fastest.
Arguments:
- green_rows: bfloat16 [128, 65536], P('groups', 'chol'), parts along dimension 0, may hold values from -6 to 6
- factors: bfloat16 [5120, 65536], P(None, 'chol'), may hold values from -0.03125 to 0.03125
- noise_draws: float32 [128, 5120], P('groups', 'chol'), parts along dimension 0, may hold values from -6 to 6
Outputs:
- potential: float32 [128, 65536], P('groups', 'chol'), parts along dimension 0
- log_weight: float32 [128], P(('groups', 'chol')), parts along dimension 0
The draws below stay inside these ranges and needn't reach their ends.
There are 2 independent parts, one for each index of `groups`. The reference program is written for one: setup_inputs(seed, part) draws one part's arguments, and reference() takes and returns one part's arrays. A program takes and returns all parts, laid end to end along the dimension named above; an argument that names none is the same for every part. Nothing has to cross between parts.
All inputs are finite; a program needn't handle non-finite values.
Results may differ from the reference program's by a relative error of at most 0.0029.
Values may be sent and summed in bfloat16 or wider, within the bound.
A program may use at most 128 MiB of HBM per device.

```python
import math
import jax
import jax.numpy as jnp
from jax import lax

NCHOL = 5120
PAIRS = 65536
WALKERS = 64


def strengthened(array, stream_key, source, target, blocks, factor):
    def block_of(position):
        return (jnp.arange(array.shape[position]) // (array.shape[position] // blocks)).reshape((-1,) + (1,) * (array.ndim - 1 - position))

    one_side = jax.random.permutation(stream_key, blocks)[block_of(target)]
    other_side = (block_of(target) + blocks // 2) % blocks
    return jnp.where((block_of(source) == one_side) | (block_of(source) == other_side), factor * array, array)


def block_scale(key, dims, cuts, smallest, top_value):
    def one(dim, shards_of):
        steps = jax.random.uniform(jax.random.fold_in(jax.random.fold_in(key, 6), dim), (shards_of,), jnp.float32, smallest / len(cuts), top_value / len(cuts))
        return jnp.repeat(jnp.exp(steps), dims[dim] // shards_of).reshape((-1,) + (1,) * (len(dims) - dim - 1))

    loudness = one(*cuts[0])
    for cut in cuts[1:]:
        loudness = loudness * one(*cut)
    return loudness


def gaussian(own_key, dims, scale, most, cuts=(), dtype=jnp.bfloat16):
    entries = scale * jax.random.normal(own_key, dims, jnp.float32)
    if cuts:
        entries = entries * block_scale(own_key, dims, cuts, -0.22, 0.18)
    return jnp.clip(entries, -most, most).astype(dtype)


def noise_with(own_key, shape, spread, bound, pieces, heavy, held_as=jnp.bfloat16):
    result = spread * jax.random.normal(own_key, shape, jnp.float32)
    if pieces:
        result = result * block_scale(own_key, shape, pieces, -0.22, 0.18)
    return jnp.clip(strengthened(result, jax.random.fold_in(own_key, 3), *heavy), -bound, bound).astype(held_as)


def setup_inputs(seed: int = 0, part: int = 0) -> dict:
    key_list = jax.random.split(jax.random.key(seed), 4)
    part_keys = jax.random.split(jax.random.fold_in(key_list[3], part), 4)
    return {
        "green_rows": gaussian(part_keys[0], (WALKERS, PAIRS), 1.0, 6.0, ((1, 16),)),
        "factors": noise_with(key_list[1], (NCHOL, PAIRS), PAIRS ** -0.5, 0.03125, ((1, 16),), (1, 0, 16, 2.0)),
        "noise_draws": gaussian(part_keys[2], (WALKERS, NCHOL), 1.0, 6.0, ((1, 16),), jnp.float32),
    }


def reference(green_rows, factors, noise_draws):
    forces = lax.dot_general(green_rows, factors, (((1,), (1,)), ((), ())), preferred_element_type=jnp.float32)
    capped = jnp.tanh(forces)
    fields = noise_draws - capped
    potential = jnp.dot(fields.astype(jnp.bfloat16), factors, preferred_element_type=jnp.float32)
    log_weight = lax.optimization_barrier(jnp.sum(fields * capped - 0.5 * capped * capped, axis=1)) / math.sqrt(NCHOL)
    return (potential, log_weight)
```

```python
import functools
import math

import jax
import jax.numpy as jnp
from jax import lax
from jax.experimental import pallas as pl
from jax.experimental.pallas import tpu as pltpu
from jax.sharding import PartitionSpec as P

MESH = pl.DeviceIdType.MESH
STAGES = 4


def flip(a, b, bits):
    total = 0
    for bit in range(bits):
        x = lax.rem(lax.div(a, 2**bit), 2)
        y = lax.rem(lax.div(b, 2**bit), 2) if not isinstance(b, int) else (b >> bit) & 1
        total = total + (x + y - 2 * x * y) * 2**bit
    return total


def kernel(n, pack, green, factors, noise, pot, logw, fac, own, d2d_out, d2d_in, rs_in, ag, nz,
           lhs, lw, lws, fac_sem, ds, dr, rs, rr, gs, gr, fs, fr, ls, lr, ps, pr):
    chips = n // 2
    bits = chips.bit_length() - 1
    total = factors.shape[0]
    nv = total // n
    half = nv // pack
    walkers = green.shape[0]
    me = lax.axis_index("chol")
    chip, core = lax.div(me, 2), lax.rem(me, 2)
    other = 1 - core
    partner = chip * 2 + other

    def peer(k):
        return flip(chip, k, bits) * 2 + core

    def load(i):
        k = chips - 1 - i
        rows = pl.ds(pl.multiple_of(flip(chip, k, bits) * (2 * nv), 2 * nv), 2 * nv)
        return pltpu.make_async_copy(factors.at[rows, :], fac.at[rows, :], fac_sem.at[k])

    def start_load(i, c):
        load(i).start()
        return c

    lax.fori_loop(0, chips, start_load, 0)

    barrier = pltpu.get_barrier_semaphore()
    pl.semaphore_signal(barrier, inc=1, device_id={"chol": partner}, device_id_type=MESH)

    def greet(k, c):
        pl.semaphore_signal(barrier, inc=1, device_id={"chol": peer(k)}, device_id_type=MESH)
        return c

    lax.fori_loop(1, chips, greet, 0)
    turned = noise[...].T
    nz[...] = jnp.concatenate([turned[j * half:(j + 1) * half] for j in range(pack)], axis=1)
    def remote(src, dst, s, r, to):
        return pltpu.make_async_remote_copy(
            src_ref=src, dst_ref=dst, send_sem=s, recv_sem=r,
            device_id={"chol": to}, device_id_type=MESH)

    def d2d(k):
        return remote(d2d_out.at[k], d2d_in.at[k], ds.at[k], dr.at[k], partner)

    def scatter(k):
        return remote(own.at[k], rs_in.at[k], rs.at[k], rr.at[k], peer(k))

    def partial(k, which):
        base = (flip(chip, k, bits) * 2 + which) * nv
        parts = []
        for j in range(pack):
            rows = pl.ds(pl.multiple_of(base + j * half, 16), half)
            parts.append(lax.dot_general(fac[rows, :], green[...], (((1,), (1,)), ((), ())),
                                         preferred_element_type=jnp.float32))
        return jnp.concatenate(parts, axis=1) if pack > 1 else parts[0]

    def finish(k):
        d2d(k).wait_recv()
        own[k] = own[k] + d2d_in[k]

    def step(i, c):
        k = chips - 1 - i
        load(i).wait()
        d2d_out[k] = partial(k, other)
        d2d(k).start()

        finish(k + 1)
        scatter(k + 1).start()
        own[k] = partial(k, core)
        return c

    load(0).wait()
    d2d_out[chips - 1] = partial(chips - 1, other)
    pl.semaphore_wait(barrier, chips)
    d2d(chips - 1).start()
    own[chips - 1] = partial(chips - 1, core)
    lax.fori_loop(1, chips, step, 0)
    finish(0)

    def gather_sum(k, acc):
        scatter(k).wait_recv()
        return acc + rs_in[k]

    forces = lax.fori_loop(1, chips, gather_sum, own[0])
    capped = jnp.tanh(forces)
    fields = nz[...] - capped

    def spread(k):
        mine = ag.at[0, core]
        return remote(mine, ag.at[k, core], gs.at[k], gr.at[k], peer(k))

    def forward(k):
        return remote(ag.at[k, core], ag.at[k, core], fs.at[k], fr.at[k], partner)

    def forward_in(k):
        return remote(ag.at[k, other], ag.at[k, other], fs.at[k], fr.at[k], partner)

    def tell(k):
        return remote(lw.at[0], lw.at[k], ls.at[k], lr.at[k], peer(k))

    pair_sum = remote(lws.at[0], lws.at[1], ps, pr, partner)

    ag[0, core] = fields.astype(jnp.bfloat16)
    forward(0).start()

    def start_spread(k, c):
        spread(k).start()
        return c

    lax.fori_loop(1, chips, start_spread, 0)
    row = jnp.sum(fields * capped - 0.5 * capped * capped, axis=0, keepdims=True)
    lw[0] = jnp.broadcast_to(row, lw.shape[1:])

    def start_tell(k, c):
        tell(k).start()
        return c

    lax.fori_loop(1, chips, start_tell, 0)

    per_stage = chips // STAGES
    deep = total // STAGES
    own_stage = lax.div(chip, per_stage)
    cols = pot.shape[1]
    width = cols // 2
    halves = cols // 2 // width

    def pull(s):
        def one(k, c):
            spread(k).wait_recv()
            forward(k).start()
            return c
        lax.fori_loop(max(1, s * per_stage), (s + 1) * per_stage, one, 0)

    def settle(s):
        def one(k, c):
            forward_in(k).wait_recv()
            return c
        lax.fori_loop(s * per_stage, (s + 1) * per_stage, one, 0)

    pull(0)
    settle(0)
    for s in range(STAGES):
        plane = flip(own_stage, s, 2)
        blocks = []
        for m in range(per_stage):
            k = flip(plane * per_stage + m, chip, bits)
            for c in range(2):
                block = ag[k, c]
                for j in range(pack):
                    blocks.append(block[:, j * walkers:(j + 1) * walkers])
        lhs[...] = jnp.concatenate(blocks, axis=0).T
        rows = pl.ds(pl.multiple_of(plane * deep, deep), deep)

        def column(t, c, s=s, rows=rows):
            at = pl.ds(pl.multiple_of(t * width, width), width)
            value = jnp.dot(lhs[...], fac[rows, at], preferred_element_type=jnp.float32)
            pot[:, at] = value if s == 0 else pot[:, at] + value
            return c

        lax.fori_loop(0, halves, column, 0)
        if s + 1 < STAGES:
            pull(s + 1)
        if s == STAGES - 2:
            def add(k, acc):
                tell(k).wait_recv()
                return acc + lw[k]
            lws[0] = lax.fori_loop(1, chips, add, lw[0])
            pair_sum.start()
        lax.fori_loop(halves, 2 * halves, column, 0)
        if s + 1 < STAGES:
            settle(s + 1)

    pair_sum.wait()
    packed = lws[0, 0:1, :] + lws[1, 0:1, :]
    row = packed[:, 0:walkers]
    for j in range(1, pack):
        row = row + packed[:, j * walkers:(j + 1) * walkers]
    per = walkers // n
    lane = lax.broadcasted_iota(jnp.int32, (1, walkers), 1)
    spot = lax.broadcasted_iota(jnp.int32, (1, per), 1)
    mine = jnp.zeros((1, per), jnp.float32)
    for j in range(per):
        one = jnp.sum(jnp.where(lane == me * per + j, row, 0.0), axis=1, keepdims=True)
        mine = jnp.where(spot == j, one, mine)
    logw[...] = (mine / math.sqrt(total)).reshape(per)

    d2d(0).wait_send()
    forward(0).wait_send()

    def drain(k, c):
        d2d(k).wait_send()
        scatter(k).wait_send()
        spread(k).wait_send()
        forward(k).wait_send()
        tell(k).wait_send()
        return c

    lax.fori_loop(1, chips, drain, 0)


def solution(mesh):
    n = mesh.shape["chol"]

    def per_device(green, factors, noise):
        walkers, cols = green.shape
        total = factors.shape[0]
        chips = n // 2
        pack = max(1, 128 // walkers)
        half, lanes = total // n // pack, walkers * pack
        vmem = pl.BlockSpec(memory_space=pltpu.VMEM)
        dma = pltpu.SemaphoreType.DMA
        block = pltpu.VMEM((chips, half, lanes), jnp.float32)
        pot, logw = pl.pallas_call(
            functools.partial(kernel, n, pack),
            out_shape=(jax.ShapeDtypeStruct((walkers, cols), jnp.float32),
                       jax.ShapeDtypeStruct((walkers // n,), jnp.float32)),
            in_specs=[vmem, pl.BlockSpec(memory_space=pl.ANY), vmem],
            out_specs=(vmem, vmem),
            scratch_shapes=[
                pltpu.VMEM(factors.shape, jnp.bfloat16),
                block, block, block, block,
                pltpu.VMEM((chips, 2, half, lanes), jnp.bfloat16),
                pltpu.VMEM((half, lanes), jnp.float32),
                pltpu.VMEM((walkers, total // STAGES), jnp.bfloat16),
                pltpu.VMEM((chips, 8, lanes), jnp.float32),
                pltpu.VMEM((2, 8, lanes), jnp.float32),
            ] + [dma((chips,))] * 11 + [dma, dma],
            compiler_params=pltpu.CompilerParams(
                collective_id=0, has_side_effects=True, vmem_limit_bytes=67043328),
        )(green, factors, noise)
        return pot, logw

    return jax.shard_map(
        per_device,
        mesh=mesh,
        in_specs=(P("groups", "chol"), P(None, "chol"), P("groups", "chol")),
        out_specs=(P("groups", "chol"), P(("groups", "chol"))),
        check_vma=False,
    )
```

```python
import functools
import math

import jax
import jax.numpy as jnp
from jax import lax
from jax.experimental import pallas as pl
from jax.experimental.pallas import tpu as pltpu
from jax.sharding import PartitionSpec as P

MESH = pl.DeviceIdType.MESH


def flip(a, b, bits):
    total = 0
    for bit in range(bits):
        x = lax.rem(lax.div(a, 2**bit), 2)
        y = lax.rem(lax.div(b, 2**bit), 2) if not isinstance(b, int) else (b >> bit) & 1
        total = total + (x + y - 2 * x * y) * 2**bit
    return total


def kernel(n, pack, waves, green, factors, noise, pot, logw,
           grn, nzi, fac, part, d2d_in, own, rs_in, far_out, far_in, ag, nz, lhs, lw, lws,
           in_sem, fac_sem, ds, dr, rs, rr, gs, gr, fs, fr, ls, lr, ps, pr):
    chips = n // 2
    bits = chips.bit_length() - 1
    pairs = chips // 2
    total, cols = factors.shape
    nv = total // n
    nw = nv // waves
    half = nw // pack
    walkers = green.shape[0]
    deep = 4 * nw
    me = lax.axis_index("chol")
    chip, core = lax.div(me, 2), lax.rem(me, 2)
    other = 1 - core
    partner = chip * 2 + other

    def peer(k):
        return flip(chip, k, bits) * 2 + core

    def at(w, k):
        return w * chips + k

    def base(w, p):
        return pl.multiple_of((w * pairs + p) * deep, deep)

    def load(w, p, b, c):
        src = (flip(chip, 2 * p + b, bits) * 2 + c) * nv + w * nw
        return pltpu.make_async_copy(
            factors.at[pl.ds(pl.multiple_of(src, nw), nw), :],
            fac.at[pl.ds(pl.multiple_of(base(w, p) + (2 * b + c) * nw, nw), nw), :],
            fac_sem.at[2 * b + c, w * pairs + p])

    green_in = pltpu.make_async_copy(green, grn, in_sem.at[0])
    noise_in = pltpu.make_async_copy(noise, nzi, in_sem.at[1])
    green_in.start()
    steps = waves * pairs

    def where(t):
        return lax.div(t, pairs), pairs - 1 - lax.rem(t, pairs)

    def start_load(t, c):
        w, p = where(t)
        for b in (0, 1):
            for e in range(2):
                load(w, p, b, e).start()
        return c

    start_load(0, 0)
    noise_in.start()
    lax.fori_loop(1, steps, start_load, 0)

    barrier = pltpu.get_barrier_semaphore()
    pl.semaphore_signal(barrier, inc=1, device_id={"chol": partner}, device_id_type=MESH)

    def greet(k, c):
        pl.semaphore_signal(barrier, inc=1, device_id={"chol": peer(k)}, device_id_type=MESH)
        return c

    lax.fori_loop(1, chips, greet, 0)

    def remote(src, dst, s, r, to):
        return pltpu.make_async_remote_copy(
            src_ref=src, dst_ref=dst, send_sem=s, recv_sem=r,
            device_id={"chol": to}, device_id_type=MESH)

    def d2d(w, k):
        q = at(w, k)
        return remote(part.at[q, other], d2d_in.at[q], ds.at[q], dr.at[q], partner)

    def near(w, k):
        q = at(w, k)
        return remote(own.at[q], rs_in.at[q], rs.at[q], rr.at[q], peer(k))

    def far(w, k):
        q = at(w, k)
        return remote(far_out.at[q], far_in.at[q], rs.at[q], rr.at[q], peer(k))

    def pack_rows(o):
        rows = [o[j * half:(j + 1) * half] for j in range(pack)]
        return jnp.concatenate(rows, axis=1) if pack > 1 else rows[0]

    def product(w, p):
        for b in range(2):
            for e in range(2):
                load(w, p, b, e).wait()
        o = lax.dot_general(fac[pl.ds(base(w, p), deep), :], grn[...], (((1,), (1,)), ((), ())),
                            preferred_element_type=jnp.float32)
        for b in range(2):
            for e in range(2):
                part[at(w, 2 * p + b), e] = pack_rows(o[(2 * b + e) * nw:(2 * b + e + 1) * nw])

    def swap(w, p):
        for b in (1, 0):
            d2d(w, 2 * p + b).start()

    def reduced(w, k):
        q = at(w, k)
        d2d(w, k).wait_recv()
        return part[q, core] + d2d_in[q]

    def send_near(w, k):
        own[at(w, k)] = reduced(w, k)
        near(w, k).start()

    def send_far(w, k):
        far_out[at(w, k)] = reduced(w, k).astype(jnp.bfloat16)
        far(w, k).start()

    def send_pair(w, p):
        @pl.when(p >= 2)
        def _():
            send_far(w, 2 * p + 1)
            send_far(w, 2 * p)

        @pl.when(p < 2)
        def _():
            send_near(w, 2 * p + 1)

        @pl.when(p == 1)
        def _():
            send_near(w, 2 * p)

        @pl.when(p == 0)
        def _():
            own[at(w, 0)] = reduced(w, 0)

    def direct(k):
        return k < 4 or k % 2 == 0

    def spread(w, k):
        return remote(ag.at[w, 0, core], ag.at[w, k, core], gs.at[w, k], gr.at[w, k], peer(k))

    def relay(w, k):
        return remote(ag.at[w, k - 1, core], ag.at[w, k, core], gs.at[w, k], gr.at[w, k], peer(1))

    def forward(w, k):
        return remote(ag.at[w, k, core], ag.at[w, k, core], fs.at[w, k], fr.at[w, k], partner)

    def forward_in(w, k):
        return remote(ag.at[w, k, other], ag.at[w, k, other], fs.at[w, k], fr.at[w, k], partner)

    def tell(k):
        return remote(lw.at[0], lw.at[k], ls.at[k], lr.at[k], peer(k))

    pair_sum = remote(lws.at[0], lws.at[1], ps, pr, partner)
    order = [p for p in (0, 1, 3, 2) if p < pairs] + list(range(4, pairs))

    def combine(w):
        def near_sum(k, acc):
            near(w, k).wait_recv()
            return acc + rs_in[at(w, k)]

        def far_sum(k, acc):
            far(w, k).wait_recv()
            return acc + far_in[at(w, k)].astype(jnp.float32)

        forces = lax.fori_loop(4, chips, far_sum, own[at(w, 0)])
        forces = lax.fori_loop(1, 4, near_sum, forces)
        capped = jnp.tanh(forces)
        fields = nz[w] - capped
        ag[w, 0, core] = fields.astype(jnp.bfloat16)
        forward(w, 0).start()
        for p in order:
            for k in (2 * p, 2 * p + 1):
                if k and direct(k):
                    spread(w, k).start()
        row = jnp.sum(fields * capped - 0.5 * capped * capped, axis=0, keepdims=True)
        row = jnp.broadcast_to(row, lw.shape[1:])
        lw[0] = row if w == 0 else lw[0] + row
        if w == waves - 1:
            def start_tell(k, c):
                tell(k).start()
                return c

            lax.fori_loop(1, chips, start_tell, 0)

    def pull(w, ks):
        for k in ks:
            spread(w, k).wait_recv()
            forward(w, k).start()
            if k >= 4 and k % 2 == 0:
                relay(w, k + 1).start()

    def settle(w, p):
        for k in (2 * p, 2 * p + 1):
            forward_in(w, k).wait_recv()

    def stage(w, p):
        blocks = []
        for k in (2 * p, 2 * p + 1):
            for e in range(2):
                block = ag[w, k, e]
                for j in range(pack):
                    blocks.append(block[:, j * walkers:(j + 1) * walkers])
        lhs[...] = jnp.concatenate(blocks, axis=0).T
        value = jnp.dot(lhs[...], fac[pl.ds(base(w, p), deep), :], preferred_element_type=jnp.float32)
        pot[...] = value if w == 0 and p == order[0] else pot[...] + value

    green_in.wait()

    def step(t, c):
        w, p = where(t)
        product(w, p)

        @pl.when(t == 0)
        def _():
            pl.semaphore_wait(barrier, chips)

        swap(w, p)

        @pl.when(t > 0)
        def _():
            send_pair(*where(t - 1))

        @pl.when(t == 0)
        def _():
            noise_in.wait()
            turned = nzi[...].T
            for v in range(waves):
                nz[v] = pack_rows(turned[v * nw:(v + 1) * nw])

        for v in range(waves - 1):
            @pl.when(t == (v + 1) * pairs + 1)
            def _(v=v):
                combine(v)
        return c

    lax.fori_loop(0, steps, step, 0)
    evens = [k for p in order[2:] for k in (2 * p,)]
    odds = [k + 1 for k in evens]
    if waves == 1:
        send_pair(0, 0)
        combine(0)
    for w in range(waves):
        last = w == waves - 1
        pull(w, [1, 2, 3] + evens)
        if not last:
            send_pair(w + 1, 0)
        for i, p in enumerate(order):
            if i == (1 if last else 2):
                pull(w, odds)
            settle(w, p)
            stage(w, p)
            if not last and i == 1:
                combine(w + 1)
            if last and i == len(order) - 2:
                def add(k, acc):
                    tell(k).wait_recv()
                    return acc + lw[k]
                lws[0] = lax.fori_loop(1, chips, add, lw[0])
                pair_sum.start()

    pair_sum.wait()
    packed = lws[0, 0:1, :] + lws[1, 0:1, :]
    row = packed[:, 0:walkers]
    for j in range(1, pack):
        row = row + packed[:, j * walkers:(j + 1) * walkers]
    per = walkers // n
    lane = lax.broadcasted_iota(jnp.int32, (1, walkers), 1)
    spot = lax.broadcasted_iota(jnp.int32, (8, 128), 1)
    mine = jnp.zeros((8, 128), jnp.float32)
    for j in range(per):
        one = jnp.sum(jnp.where(lane == me * per + j, row, 0.0), axis=1, keepdims=True)
        mine = jnp.where(spot == j, one, mine)
    logw[...] = mine / math.sqrt(total)

    for w in range(waves):
        d2d(w, 0).wait_send()
        forward(w, 0).wait_send()

        def drain_near(k, c, w=w):
            near(w, k).wait_send()
            return c

        def drain_far(k, c, w=w):
            far(w, k).wait_send()
            return c

        def drain(k, c, w=w):
            d2d(w, k).wait_send()
            spread(w, k).wait_send()
            forward(w, k).wait_send()
            return c

        lax.fori_loop(1, 4, drain_near, 0)
        lax.fori_loop(4, chips, drain_far, 0)
        lax.fori_loop(1, chips, drain, 0)

    def drain_tell(k, c):
        tell(k).wait_send()
        return c

    lax.fori_loop(1, chips, drain_tell, 0)


def hand_over(pot, logw, pot_out, logw_out):
    pot_out[...] = pot[...]
    logw_out[...] = logw[0:1, 0:logw_out.shape[0]].reshape(logw_out.shape)


def solution(mesh):
    n = mesh.shape["chol"]

    def per_device(green, factors, noise):
        walkers, cols = green.shape
        total = factors.shape[0]
        chips = n // 2
        nv = total // n
        pack = max(1, 128 // walkers)
        waves = 2 if nv % (32 * pack) == 0 else 1
        half, lanes = nv // waves // pack, walkers * pack
        vmem = pl.BlockSpec(memory_space=pltpu.VMEM)
        hbm = pl.BlockSpec(memory_space=pltpu.HBM)
        dma = pltpu.SemaphoreType.DMA
        block = (waves * chips, half, lanes)
        pot, logw = pl.pallas_call(
            functools.partial(kernel, n, pack, waves),
            out_shape=(pltpu.VMEM((walkers, cols), jnp.float32), pltpu.VMEM((8, 128), jnp.float32)),
            in_specs=[hbm, hbm, hbm],
            out_specs=(vmem, vmem),
            scratch_shapes=[
                pltpu.VMEM(green.shape, jnp.bfloat16),
                pltpu.VMEM(noise.shape, jnp.float32),
                pltpu.VMEM(factors.shape, jnp.bfloat16),
                pltpu.VMEM((waves * chips, 2, half, lanes), jnp.float32),
                pltpu.VMEM(block, jnp.float32),
                pltpu.VMEM(block, jnp.float32),
                pltpu.VMEM(block, jnp.float32),
                pltpu.VMEM(block, jnp.bfloat16),
                pltpu.VMEM(block, jnp.bfloat16),
                pltpu.VMEM((waves, chips, 2, half, lanes), jnp.bfloat16),
                pltpu.VMEM((waves, half, lanes), jnp.float32),
                pltpu.VMEM((walkers, 4 * (nv // waves)), jnp.bfloat16),
                pltpu.VMEM((chips, 8, lanes), jnp.float32),
                pltpu.VMEM((2, 8, lanes), jnp.float32),
                dma((2,)), dma((4, waves * chips // 2)),
            ] + [dma((waves * chips,))] * 4 + [dma((waves, chips))] * 4 + [dma((chips,))] * 2 + [dma, dma],
            compiler_params=pltpu.CompilerParams(
                collective_id=0, has_side_effects=True, vmem_limit_bytes=58 * 2**20),
        )(green, factors, noise)
        return pl.pallas_call(
            hand_over,
            out_shape=(jax.ShapeDtypeStruct((walkers, cols), jnp.float32),
                       jax.ShapeDtypeStruct((walkers // n,), jnp.float32)),
            in_specs=[vmem, vmem],
            out_specs=(vmem, vmem),
            compiler_params=pltpu.CompilerParams(vmem_limit_bytes=4 * 2**20),
        )(pot, logw)

    return jax.shard_map(
        per_device,
        mesh=mesh,
        in_specs=(P("groups", "chol"), P(None, "chol"), P("groups", "chol")),
        out_specs=(P("groups", "chol"), P(("groups", "chol"))),
        check_vma=False,
    )
```

```python
import functools
import math

import jax
import jax.numpy as jnp
from jax import lax
from jax.experimental import pallas as pl
from jax.experimental.pallas import tpu as pltpu
from jax.sharding import PartitionSpec as P

MESH = pl.DeviceIdType.MESH


def flip(a, b, bits):
    total = 0
    for bit in range(bits):
        x = lax.rem(lax.div(a, 2**bit), 2)
        y = lax.rem(lax.div(b, 2**bit), 2) if not isinstance(b, int) else (b >> bit) & 1
        total = total + (x + y - 2 * x * y) * 2**bit
    return total


def kernel(n, pack, waves, green, factors, noise, pot, logw,
           grn, nzi, fac, part, d2d_in, own, rs_out, rs_in, ag, nz, lhs, lw, lws,
           in_sem, fac_sem, ds, dr, rs, rr, gs, gr, fs, fr, ls, lr, ps, pr):
    chips = n // 2
    bits = chips.bit_length() - 1
    pairs = chips // 2
    total, cols = factors.shape
    nv = total // n
    nw = nv // waves
    half = nw // pack
    walkers = green.shape[0]
    deep = 4 * nw
    me = lax.axis_index("chol")
    chip, core = lax.div(me, 2), lax.rem(me, 2)
    other = 1 - core
    partner = chip * 2 + other

    def peer(k):
        return flip(chip, k, bits) * 2 + core

    def at(w, k):
        return w * chips + k

    def base(w, p):
        return pl.multiple_of((w * pairs + p) * deep, deep)

    def member(p, b):
        if isinstance(p, int):
            return p // 2 * 4 + p % 2 + 2 * b
        return lax.div(p, 2) * 4 + lax.rem(p, 2) + 2 * b

    def load(w, p, b, c):
        src = (flip(chip, member(p, b), bits) * 2 + c) * nv + w * nw
        return pltpu.make_async_copy(
            factors.at[pl.ds(pl.multiple_of(src, nw), nw), :],
            fac.at[pl.ds(pl.multiple_of(base(w, p) + (2 * b + c) * nw, nw), nw), :],
            fac_sem.at[w * pairs + p])

    green_in = pltpu.make_async_copy(green, grn, in_sem.at[0])
    noise_in = pltpu.make_async_copy(noise, nzi, in_sem.at[1])
    green_in.start()
    steps = waves * pairs

    def where(t):
        return lax.div(t, pairs), pairs - 1 - lax.rem(t, pairs)

    def start_load(t, c):
        w, p = where(t)
        for b in (0, 1):
            for e in range(2):
                load(w, p, b, e).start()
        return c

    start_load(0, 0)
    noise_in.start()
    lax.fori_loop(1, steps, start_load, 0)

    barrier = pltpu.get_barrier_semaphore()
    pl.semaphore_signal(barrier, inc=1, device_id={"chol": partner}, device_id_type=MESH)

    def greet(k, c):
        pl.semaphore_signal(barrier, inc=1, device_id={"chol": peer(k)}, device_id_type=MESH)
        return c

    lax.fori_loop(1, chips, greet, 0)

    def remote(src, dst, s, r, to):
        return pltpu.make_async_remote_copy(
            src_ref=src, dst_ref=dst, send_sem=s, recv_sem=r,
            device_id={"chol": to}, device_id_type=MESH)

    def arrived(ref, sem):
        pltpu.make_async_copy(ref, ref, sem).wait()

    def blocks_of(count):
        return rs_in.at[pl.ds(0, count)]

    def d2d(w, p, b):
        q = at(w, member(p, b))
        return remote(part.at[q, other], d2d_in.at[q], ds, dr.at[w * pairs + p], partner)

    def send(w, k, to, group):
        q = at(w, k)
        return remote(rs_out.at[q], rs_in.at[q], rs, rr.at[w, group], peer(to))

    def pack_rows(o):
        rows = [o[j * half:(j + 1) * half] for j in range(pack)]
        return jnp.concatenate(rows, axis=1) if pack > 1 else rows[0]

    def product(w, p):
        arrived(fac.at[pl.ds(base(w, p), deep), :], fac_sem.at[w * pairs + p])
        o = lax.dot_general(fac[pl.ds(base(w, p), deep), :], grn[...], (((1,), (1,)), ((), ())),
                            preferred_element_type=jnp.float32)
        for b in range(2):
            for e in range(2):
                part[at(w, member(p, b)), e] = pack_rows(o[(2 * b + e) * nw:(2 * b + e + 1) * nw])

    def swap(w, p):
        for b in (1, 0):
            d2d(w, p, b).start()

    def swapped(w, p):
        arrived(d2d_in.at[pl.ds(0, 2)], dr.at[w * pairs + p])

    def reduced(w, k):
        q = at(w, k)
        return part[q, core] + d2d_in[q]

    def push(w, k, to, group, value):
        rs_out[at(w, k)] = value.astype(jnp.bfloat16)
        send(w, k, to, group).start()

    def service(w, p):
        @pl.when((p >= 2) & (lax.rem(p, 2) == 1))
        def _():
            swapped(w, p)
            for b in (1, 0):
                k = member(p, b)
                push(w, k, 1, lax.div(p, 2), reduced(w, k))

        @pl.when(p == 1)
        def _():
            swapped(w, p)
            for k in (3, 1):
                push(w, k, k, 0, reduced(w, k))

    def service_far(w, p):
        @pl.when((p >= 2) & (lax.rem(p, 2) == 0))
        def _():
            swapped(w, p)
            arrived(blocks_of(2), rr.at[w, lax.div(p, 2)])
            for b in (1, 0):
                k = member(p, b)
                push(w, k, k, 0, reduced(w, k) + rs_in[at(w, k + 1)].astype(jnp.float32))

    def service_last(w):
        swapped(w, 0)
        push(w, 2, 2, 0, reduced(w, 2))
        own[w] = reduced(w, 0)

    evens = list(range(4, chips, 2))
    odds = [k + 1 for k in evens]

    def got(k):
        return 0 if k < 4 else 1 if k % 2 else k // 2

    def spread(w, k):
        return remote(ag.at[w, 0, core], ag.at[w, k, core], gs, gr.at[w, got(k)], peer(k))

    def relay(w, k):
        return remote(ag.at[w, k - 1, core], ag.at[w, k, core], gs, gr.at[w, got(k)], peer(1))

    def forward(w, k):
        return remote(ag.at[w, k, core], ag.at[w, k, core], fs, fr.at[w, k // 4 * 2 + k % 2], partner)

    def tell(k):
        return remote(lw.at[0], lw.at[k], ls, lr, peer(k))

    pair_sum = remote(lws.at[0], lws.at[1], ps, pr, partner)
    order = range(pairs)

    def combine(w):
        forces = own[w]
        arrived(blocks_of(3 + len(evens)), rr.at[w, 0])
        for k in evens + [1, 2, 3]:
            forces = forces + rs_in[at(w, k)].astype(jnp.float32)
        capped = jnp.tanh(forces)
        fields = nz[w] - capped
        ag[w, 0, core] = fields.astype(jnp.bfloat16)
        for k in evens[::-1] + [2, 3, 1]:
            spread(w, k).start()
        forward(w, 0).start()
        row = jnp.sum(fields * capped - 0.5 * capped * capped, axis=0, keepdims=True)
        row = jnp.broadcast_to(row, lw.shape[1:])
        lw[0] = row if w == 0 else lw[0] + row
        if w == waves - 1:
            def start_tell(k, c):
                tell(k).start()
                return c

            lax.fori_loop(1, chips, start_tell, 0)

    def pull_near(w):
        arrived(blocks_of(3), gr.at[w, 0])
        for k in (1, 2, 3):
            forward(w, k).start()

    def pull_evens(w):
        for k in evens:
            arrived(blocks_of(1), gr.at[w, got(k)])
            relay(w, k + 1).start()
            forward(w, k).start()

    def pull_odds(w):
        if odds:
            arrived(blocks_of(len(odds)), gr.at[w, 1])
        for k in odds:
            forward(w, k).start()

    def settle(w, p):
        arrived(blocks_of(2), fr.at[w, p])

    def stage(w, p):
        blocks = []
        for b in range(2):
            for e in range(2):
                block = ag[w, member(p, b), e]
                for j in range(pack):
                    blocks.append(block[:, j * walkers:(j + 1) * walkers])
        lhs[...] = jnp.concatenate(blocks, axis=0).T
        value = jnp.dot(lhs[...], fac[pl.ds(base(w, p), deep), :], preferred_element_type=jnp.float32)
        pot[...] = value if w == 0 and p == order[0] else pot[...] + value

    green_in.wait()

    def step(t, c):
        w, p = where(t)
        product(w, p)

        @pl.when(t == 0)
        def _():
            pl.semaphore_wait(barrier, chips)

        swap(w, p)

        @pl.when(t > 1)
        def _():
            service_far(*where(t - 2))

        @pl.when(t > 0)
        def _():
            service(*where(t - 1))

        for v in range(waves - 1):
            @pl.when(t == (v + 1) * pairs)
            def _(v=v):
                service_last(v)

        @pl.when(t == 0)
        def _():
            noise_in.wait()
            turned = nzi[...].T
            for v in range(waves):
                nz[v] = pack_rows(turned[v * nw:(v + 1) * nw])

        for v in range(waves - 1):
            @pl.when(t == (v + 1) * pairs + pairs // 2)
            def _(v=v):
                combine(v)
        return c

    lax.fori_loop(0, steps, step, 0)
    def settle_weights():
        arrived(lw.at[pl.ds(1, chips - 1)], lr)
        acc = lw[0]
        for k in range(1, chips):
            acc = acc + lw[k]
        lws[0] = acc
        pair_sum.start()

    def write_weights():
        pair_sum.wait()
        packed = lws[0, 0:1, :] + lws[1, 0:1, :]
        row = packed[:, 0:walkers]
        for j in range(1, pack):
            row = row + packed[:, j * walkers:(j + 1) * walkers]
        per = walkers // n
        lane = lax.broadcasted_iota(jnp.int32, (1, walkers), 1)
        spot = lax.broadcasted_iota(jnp.int32, (8, 128), 1)
        mine = jnp.zeros((8, 128), jnp.float32)
        for j in range(per):
            one = jnp.sum(jnp.where(lane == me * per + j, row, 0.0), axis=1, keepdims=True)
            mine = jnp.where(spot == j, one, mine)
        logw[...] = mine / math.sqrt(total)

    if waves == 1:
        service_last(0)
        combine(0)
    for w in range(waves):
        last = w == waves - 1
        if last:
            pull_evens(w)
            pull_near(w)
        else:
            pull_near(w)
            service_last(w + 1)
            pull_evens(w)
        for i, p in enumerate(order):
            settle(w, p)
            stage(w, p)
            if not last and i == 1:
                combine(w + 1)
            if last and i == 0:
                settle_weights()
            if i == (0 if last else 1):
                pull_odds(w)
            if last and i == len(order) - 2:
                write_weights()

    arrived(d2d_in, ds)
    arrived(blocks_of(waves * (chips - 1)), rs)
    arrived(blocks_of(waves * (chips - 1)), gs)
    arrived(blocks_of(waves * chips), fs)
    arrived(lw.at[pl.ds(1, chips - 1)], ls)


def hand_over(pot, logw, pot_out, logw_out):
    pot_out[...] = pot[...]
    logw_out[...] = logw[0:1, 0:logw_out.shape[0]].reshape(logw_out.shape)


def solution(mesh):
    n = mesh.shape["chol"]

    def per_device(green, factors, noise):
        walkers, cols = green.shape
        total = factors.shape[0]
        chips = n // 2
        nv = total // n
        pack = max(1, 128 // walkers)
        waves = 2 if nv % (32 * pack) == 0 else 1
        half, lanes = nv // waves // pack, walkers * pack
        vmem = pl.BlockSpec(memory_space=pltpu.VMEM)
        hbm = pl.BlockSpec(memory_space=pltpu.HBM)
        dma = pltpu.SemaphoreType.DMA
        block = (waves * chips, half, lanes)
        pot, logw = pl.pallas_call(
            functools.partial(kernel, n, pack, waves),
            out_shape=(pltpu.VMEM((walkers, cols), jnp.float32), pltpu.VMEM((8, 128), jnp.float32)),
            in_specs=[hbm, hbm, hbm],
            out_specs=(vmem, vmem),
            scratch_shapes=[
                pltpu.VMEM(green.shape, jnp.bfloat16),
                pltpu.VMEM(noise.shape, jnp.float32),
                pltpu.VMEM(factors.shape, jnp.bfloat16),
                pltpu.VMEM((waves * chips, 2, half, lanes), jnp.float32),
                pltpu.VMEM(block, jnp.float32),
                pltpu.VMEM((waves, half, lanes), jnp.float32),
                pltpu.VMEM(block, jnp.bfloat16),
                pltpu.VMEM(block, jnp.bfloat16),
                pltpu.VMEM((waves, chips, 2, half, lanes), jnp.bfloat16),
                pltpu.VMEM((waves, half, lanes), jnp.float32),
                pltpu.VMEM((walkers, 4 * (nv // waves)), jnp.bfloat16),
                pltpu.VMEM((chips, 8, lanes), jnp.float32),
                pltpu.VMEM((2, 8, lanes), jnp.float32),
                dma((2,)), dma((waves * chips // 2,)),
                dma, dma((waves * chips // 2,)), dma, dma((waves, chips // 4)),
                dma, dma((waves, chips // 2)), dma, dma((waves, chips // 2)),
                dma, dma, dma, dma,
            ],
            compiler_params=pltpu.CompilerParams(
                collective_id=0, has_side_effects=True, vmem_limit_bytes=58 * 2**20),
        )(green, factors, noise)
        return pl.pallas_call(
            hand_over,
            out_shape=(jax.ShapeDtypeStruct((walkers, cols), jnp.float32),
                       jax.ShapeDtypeStruct((walkers // n,), jnp.float32)),
            in_specs=[vmem, vmem],
            out_specs=(vmem, vmem),
            compiler_params=pltpu.CompilerParams(vmem_limit_bytes=4 * 2**20),
        )(pot, logw)

    return jax.shard_map(
        per_device,
        mesh=mesh,
        in_specs=(P("groups", "chol"), P(None, "chol"), P("groups", "chol")),
        out_specs=(P("groups", "chol"), P(("groups", "chol"))),
        check_vma=False,
    )
```

```python
import functools
import math

import jax
import jax.numpy as jnp
from jax import lax
from jax.experimental import pallas as pl
from jax.experimental.pallas import tpu as pltpu
from jax.sharding import PartitionSpec as P

MESH = pl.DeviceIdType.MESH


def flip(a, b, bits):
    total = 0
    for bit in range(bits):
        x = lax.rem(lax.div(a, 2**bit), 2)
        y = lax.rem(lax.div(b, 2**bit), 2) if not isinstance(b, int) else (b >> bit) & 1
        total = total + (x + y - 2 * x * y) * 2**bit
    return total


def kernel(n, pack, waves, green, factors, noise, pot, logw,
           grn, nzi, fac, part, d2d_in, own, rs_out, rs_in, ag, nz, lhs, lw, lws,
           in_sem, fac_sem, ds, dr, rs, rr, gs, gr, fs, fr, ls, lr, ps, pr):
    chips = n // 2
    bits = chips.bit_length() - 1
    pairs = chips // 2
    total, cols = factors.shape
    nv = total // n
    nw = nv // waves
    half = nw // pack
    walkers = green.shape[0]
    deep = 4 * nw
    me = lax.axis_index("chol")
    chip, core = lax.div(me, 2), lax.rem(me, 2)
    other = 1 - core
    partner = chip * 2 + other

    def peer(k):
        return flip(chip, k, bits) * 2 + core

    def at(w, k):
        return w * chips + k

    def base(w, p):
        return pl.multiple_of((w * pairs + p) * deep, deep)

    def member(p, b):
        if isinstance(p, int):
            return p // 2 * 4 + p % 2 + 2 * b
        return lax.div(p, 2) * 4 + lax.rem(p, 2) + 2 * b

    def load(w, p, b, c):
        src = (flip(chip, member(p, b), bits) * 2 + c) * nv + w * nw
        return pltpu.make_async_copy(
            factors.at[pl.ds(pl.multiple_of(src, nw), nw), :],
            fac.at[pl.ds(pl.multiple_of(base(w, p) + (2 * b + c) * nw, nw), nw), :],
            fac_sem.at[w * pairs + p])

    green_in = pltpu.make_async_copy(green, grn, in_sem.at[0])
    noise_in = pltpu.make_async_copy(noise, nzi, in_sem.at[1])
    green_in.start()
    steps = waves * pairs

    def where(t):
        return lax.div(t, pairs), pairs - 1 - lax.rem(t, pairs)

    def start_load(t, c):
        w, p = where(t)
        for b in (0, 1):
            for e in range(2):
                load(w, p, b, e).start()
        return c

    start_load(0, 0)
    noise_in.start()
    lax.fori_loop(1, steps, start_load, 0)

    barrier = pltpu.get_barrier_semaphore()
    pl.semaphore_signal(barrier, inc=1, device_id={"chol": partner}, device_id_type=MESH)

    def greet(k, c):
        pl.semaphore_signal(barrier, inc=1, device_id={"chol": peer(k)}, device_id_type=MESH)
        return c

    lax.fori_loop(1, chips, greet, 0)

    def remote(src, dst, s, r, to):
        return pltpu.make_async_remote_copy(
            src_ref=src, dst_ref=dst, send_sem=s, recv_sem=r,
            device_id={"chol": to}, device_id_type=MESH)

    def arrived(ref, sem):
        pltpu.make_async_copy(ref, ref, sem).wait()

    def blocks_of(count):
        return rs_in.at[pl.ds(0, count)]

    def d2d(w, p, b):
        q = at(w, member(p, b))
        return remote(part.at[q, other], d2d_in.at[q], ds, dr.at[w * pairs + p], partner)

    def send(w, k, to, group):
        q = at(w, k)
        return remote(rs_out.at[q], rs_in.at[q], rs, rr.at[w, group], peer(to))

    def pack_rows(o):
        rows = [o[j * half:(j + 1) * half] for j in range(pack)]
        return jnp.concatenate(rows, axis=1) if pack > 1 else rows[0]

    def product(w, p):
        arrived(fac.at[pl.ds(base(w, p), deep), :], fac_sem.at[w * pairs + p])
        o = lax.dot_general(fac[pl.ds(base(w, p), deep), :], grn[...], (((1,), (1,)), ((), ())),
                            preferred_element_type=jnp.float32)
        for b in range(2):
            for e in range(2):
                part[at(w, member(p, b)), e] = pack_rows(o[(2 * b + e) * nw:(2 * b + e + 1) * nw])

    def swap(w, p):
        for b in (1, 0):
            d2d(w, p, b).start()

    def swapped(w, p):
        arrived(d2d_in.at[pl.ds(0, 2)], dr.at[w * pairs + p])

    def reduced(w, k):
        q = at(w, k)
        return part[q, core] + d2d_in[q]

    def push(w, k, to, group, value):
        rs_out[at(w, k)] = value.astype(jnp.bfloat16)
        send(w, k, to, group).start()

    def service(w, p):
        @pl.when((p >= 2) & (lax.rem(p, 2) == 1))
        def _():
            swapped(w, p)
            for b in (1, 0):
                k = member(p, b)
                push(w, k, 1, lax.div(p, 2), reduced(w, k))

        @pl.when(p == 1)
        def _():
            swapped(w, p)
            for k in (3, 1):
                push(w, k, k, 0, reduced(w, k))

    def service_far(w, p):
        @pl.when((p >= 2) & (lax.rem(p, 2) == 0))
        def _():
            swapped(w, p)
            arrived(blocks_of(2), rr.at[w, lax.div(p, 2)])
            for b in (1, 0):
                k = member(p, b)
                push(w, k, k, 0, reduced(w, k) + rs_in[at(w, k + 1)].astype(jnp.float32))

    def service_last(w):
        swapped(w, 0)
        push(w, 2, 2, 0, reduced(w, 2))
        own[w] = reduced(w, 0)

    evens = list(range(4, chips, 2))
    odds = [k + 1 for k in evens]

    def got(k):
        return 0 if k < 4 else 1 if k % 2 else k // 2

    def spread(w, k):
        return remote(ag.at[w, 0, core], ag.at[w, k, core], gs, gr.at[w, got(k)], peer(k))

    def relay(w, k):
        return remote(ag.at[w, k - 1, core], ag.at[w, k, core], gs, gr.at[w, got(k)], peer(1))

    def forward(w, k):
        return remote(ag.at[w, k, core], ag.at[w, k, core], fs, fr.at[w, k // 4 * 2 + k % 2], partner)

    def tell(k):
        return remote(lw.at[0], lw.at[k], ls, lr, peer(k))

    pair_sum = remote(lws.at[0], lws.at[1], ps, pr, partner)
    order = range(pairs)

    def combine(w):
        forces = own[w]
        arrived(blocks_of(3 + len(evens)), rr.at[w, 0])
        for k in evens + [1, 2, 3]:
            forces = forces + rs_in[at(w, k)].astype(jnp.float32)
        capped = jnp.tanh(forces)
        fields = nz[w] - capped
        ag[w, 0, core] = fields.astype(jnp.bfloat16)
        for k in evens[::-1] + [2, 3, 1] if w == waves - 1 else [2, 3, 1] + evens[::-1]:
            spread(w, k).start()
        forward(w, 0).start()
        row = jnp.sum(fields * capped - 0.5 * capped * capped, axis=0, keepdims=True)
        row = jnp.broadcast_to(row, lw.shape[1:])
        lw[0] = row if w == 0 else lw[0] + row
        if w == waves - 1:
            def start_tell(k, c):
                tell(k).start()
                return c

            lax.fori_loop(1, chips, start_tell, 0)

    def pull_near(w):
        arrived(blocks_of(3), gr.at[w, 0])
        for k in (1, 2, 3):
            forward(w, k).start()

    def pull_evens(w):
        for k in evens:
            arrived(blocks_of(1), gr.at[w, got(k)])
            relay(w, k + 1).start()
            forward(w, k).start()

    def pull_odds(w):
        if odds:
            arrived(blocks_of(len(odds)), gr.at[w, 1])
        for k in odds:
            forward(w, k).start()

    def settle(w, p):
        arrived(blocks_of(2), fr.at[w, p])

    def stage(w, p):
        blocks = []
        for b in range(2):
            for e in range(2):
                block = ag[w, member(p, b), e]
                for j in range(pack):
                    blocks.append(block[:, j * walkers:(j + 1) * walkers])
        lhs[...] = jnp.concatenate(blocks, axis=0).T
        value = jnp.dot(lhs[...], fac[pl.ds(base(w, p), deep), :], preferred_element_type=jnp.float32)
        pot[...] = value if w == 0 and p == order[0] else pot[...] + value

    green_in.wait()

    def step(t, c):
        w, p = where(t)
        product(w, p)

        @pl.when(t == 0)
        def _():
            pl.semaphore_wait(barrier, chips)

        swap(w, p)

        @pl.when(t > 1)
        def _():
            service_far(*where(t - 2))

        @pl.when(t > 0)
        def _():
            service(*where(t - 1))

        for v in range(waves - 1):
            @pl.when(t == (v + 1) * pairs)
            def _(v=v):
                service_last(v)

        @pl.when(t == 0)
        def _():
            noise_in.wait()
            turned = nzi[...].T
            for v in range(waves):
                nz[v] = pack_rows(turned[v * nw:(v + 1) * nw])

        for v in range(waves - 1):
            @pl.when(t == (v + 1) * pairs + pairs // 2)
            def _(v=v):
                combine(v)
        return c

    lax.fori_loop(0, steps, step, 0)
    def settle_weights():
        arrived(lw.at[pl.ds(1, chips - 1)], lr)
        acc = lw[0]
        for k in range(1, chips):
            acc = acc + lw[k]
        lws[0] = acc
        pair_sum.start()

    def write_weights():
        pair_sum.wait()
        packed = lws[0, 0:1, :] + lws[1, 0:1, :]
        row = packed[:, 0:walkers]
        for j in range(1, pack):
            row = row + packed[:, j * walkers:(j + 1) * walkers]
        per = walkers // n
        lane = lax.broadcasted_iota(jnp.int32, (1, walkers), 1)
        spot = lax.broadcasted_iota(jnp.int32, (8, 128), 1)
        mine = jnp.zeros((8, 128), jnp.float32)
        for j in range(per):
            one = jnp.sum(jnp.where(lane == me * per + j, row, 0.0), axis=1, keepdims=True)
            mine = jnp.where(spot == j, one, mine)
        logw[...] = mine / math.sqrt(total)

    if waves == 1:
        service_last(0)
        combine(0)
    for w in range(waves):
        last = w == waves - 1
        if last:
            pull_evens(w)
            pull_near(w)
        else:
            pull_near(w)
            service_last(w + 1)
            pull_evens(w)
        for i, p in enumerate(order):
            settle(w, p)
            stage(w, p)
            if not last and i == 0:
                combine(w + 1)
            if last and i == 0:
                settle_weights()
            if i == (0 if last else 1):
                pull_odds(w)
            if last and i == len(order) - 2:
                write_weights()

    arrived(d2d_in, ds)
    arrived(blocks_of(waves * (chips - 1)), rs)
    arrived(blocks_of(waves * (chips - 1)), gs)
    arrived(blocks_of(waves * chips), fs)
    arrived(lw.at[pl.ds(1, chips - 1)], ls)


def hand_over(pot, logw, pot_out, logw_out):
    pot_out[...] = pot[...]
    logw_out[...] = logw[0:1, 0:logw_out.shape[0]].reshape(logw_out.shape)


def solution(mesh):
    n = mesh.shape["chol"]

    def per_device(green, factors, noise):
        walkers, cols = green.shape
        total = factors.shape[0]
        chips = n // 2
        nv = total // n
        pack = max(1, 128 // walkers)
        waves = 2 if nv % (32 * pack) == 0 else 1
        half, lanes = nv // waves // pack, walkers * pack
        vmem = pl.BlockSpec(memory_space=pltpu.VMEM)
        hbm = pl.BlockSpec(memory_space=pltpu.HBM)
        dma = pltpu.SemaphoreType.DMA
        block = (waves * chips, half, lanes)
        pot, logw = pl.pallas_call(
            functools.partial(kernel, n, pack, waves),
            out_shape=(pltpu.VMEM((walkers, cols), jnp.float32), pltpu.VMEM((8, 128), jnp.float32)),
            in_specs=[hbm, hbm, hbm],
            out_specs=(vmem, vmem),
            scratch_shapes=[
                pltpu.VMEM(green.shape, jnp.bfloat16),
                pltpu.VMEM(noise.shape, jnp.float32),
                pltpu.VMEM(factors.shape, jnp.bfloat16),
                pltpu.VMEM((waves * chips, 2, half, lanes), jnp.float32),
                pltpu.VMEM(block, jnp.float32),
                pltpu.VMEM((waves, half, lanes), jnp.float32),
                pltpu.VMEM(block, jnp.bfloat16),
                pltpu.VMEM(block, jnp.bfloat16),
                pltpu.VMEM((waves, chips, 2, half, lanes), jnp.bfloat16),
                pltpu.VMEM((waves, half, lanes), jnp.float32),
                pltpu.VMEM((walkers, 4 * (nv // waves)), jnp.bfloat16),
                pltpu.VMEM((chips, 8, lanes), jnp.float32),
                pltpu.VMEM((2, 8, lanes), jnp.float32),
                dma((2,)), dma((waves * chips // 2,)),
                dma, dma((waves * chips // 2,)), dma, dma((waves, chips // 4)),
                dma, dma((waves, chips // 2)), dma, dma((waves, chips // 2)),
                dma, dma, dma, dma,
            ],
            compiler_params=pltpu.CompilerParams(
                collective_id=0, has_side_effects=True, vmem_limit_bytes=58 * 2**20),
        )(green, factors, noise)
        return pl.pallas_call(
            hand_over,
            out_shape=(jax.ShapeDtypeStruct((walkers, cols), jnp.float32),
                       jax.ShapeDtypeStruct((walkers // n,), jnp.float32)),
            in_specs=[vmem, vmem],
            out_specs=(vmem, vmem),
            compiler_params=pltpu.CompilerParams(vmem_limit_bytes=4 * 2**20),
        )(pot, logw)

    return jax.shard_map(
        per_device,
        mesh=mesh,
        in_specs=(P("groups", "chol"), P(None, "chol"), P("groups", "chol")),
        out_specs=(P("groups", "chol"), P(("groups", "chol"))),
        check_vma=False,
    )
```

```python
import functools
import math

import jax
import jax.numpy as jnp
from jax import lax
from jax.experimental import pallas as pl
from jax.experimental.pallas import tpu as pltpu
from jax.sharding import PartitionSpec as P

MESH = pl.DeviceIdType.MESH


def flip(a, b, bits):
    total = 0
    for bit in range(bits):
        x = lax.rem(lax.div(a, 2**bit), 2)
        y = lax.rem(lax.div(b, 2**bit), 2) if not isinstance(b, int) else (b >> bit) & 1
        total = total + (x + y - 2 * x * y) * 2**bit
    return total


def kernel(n, pack, waves, green, factors, noise, pot, logw,
           grn, nzi, fac, part, d2d_in, own, rs_out, rs_in, ag, nz, lhs, lw, lws,
           in_sem, fac_sem, ds, dr, rs, rr, gs, gr, fs, fr, ls, lr, ps, pr):
    chips = n // 2
    bits = chips.bit_length() - 1
    pairs = chips // 2
    total, cols = factors.shape
    nv = total // n
    nw = nv // waves
    half = nw // pack
    walkers = green.shape[0]
    deep = 4 * nw
    me = lax.axis_index("chol")
    chip, core = lax.div(me, 2), lax.rem(me, 2)
    other = 1 - core
    partner = chip * 2 + other

    def peer(k):
        return flip(chip, k, bits) * 2 + core

    def at(w, k):
        return w * chips + k

    def base(w, p):
        return pl.multiple_of((w * pairs + p) * deep, deep)

    def member(p, b):
        if isinstance(p, int):
            return p // 2 * 4 + p % 2 + 2 * b
        return lax.div(p, 2) * 4 + lax.rem(p, 2) + 2 * b

    def load(w, p, b, c):
        src = (flip(chip, member(p, b), bits) * 2 + c) * nv + w * nw
        return pltpu.make_async_copy(
            factors.at[pl.ds(pl.multiple_of(src, nw), nw), :],
            fac.at[pl.ds(pl.multiple_of(base(w, p) + (2 * b + c) * nw, nw), nw), :],
            fac_sem.at[w * pairs + p])

    green_in = pltpu.make_async_copy(green, grn, in_sem.at[0])
    noise_in = pltpu.make_async_copy(noise, nzi, in_sem.at[1])
    green_in.start()
    steps = waves * pairs

    def where(t):
        return lax.div(t, pairs), pairs - 1 - lax.rem(t, pairs)

    def start_load(t, c):
        w, p = where(t)
        for b in (0, 1):
            for e in range(2):
                load(w, p, b, e).start()
        return c

    start_load(0, 0)
    noise_in.start()
    lax.fori_loop(1, steps, start_load, 0)

    barrier = pltpu.get_barrier_semaphore()
    pl.semaphore_signal(barrier, inc=1, device_id={"chol": partner}, device_id_type=MESH)

    def greet(k, c):
        pl.semaphore_signal(barrier, inc=1, device_id={"chol": peer(k)}, device_id_type=MESH)
        return c

    lax.fori_loop(1, chips, greet, 0)

    def remote(src, dst, s, r, to):
        return pltpu.make_async_remote_copy(
            src_ref=src, dst_ref=dst, send_sem=s, recv_sem=r,
            device_id={"chol": to}, device_id_type=MESH)

    def arrived(ref, sem):
        pltpu.make_async_copy(ref, ref, sem).wait()

    def blocks_of(count):
        return rs_in.at[pl.ds(0, count)]

    def d2d(w, p, b):
        q = at(w, member(p, b))
        return remote(part.at[q, other], d2d_in.at[q], ds, dr.at[w * pairs + p], partner)

    def send(w, k, to, group):
        q = at(w, k)
        return remote(rs_out.at[q], rs_in.at[q], rs, rr.at[w, group], peer(to))

    def pack_rows(o):
        rows = [o[j * half:(j + 1) * half] for j in range(pack)]
        return jnp.concatenate(rows, axis=1) if pack > 1 else rows[0]

    def product(w, p):
        arrived(fac.at[pl.ds(base(w, p), deep), :], fac_sem.at[w * pairs + p])
        o = lax.dot_general(fac[pl.ds(base(w, p), deep), :], grn[...], (((1,), (1,)), ((), ())),
                            preferred_element_type=jnp.float32)
        for b in range(2):
            for e in range(2):
                part[at(w, member(p, b)), e] = pack_rows(o[(2 * b + e) * nw:(2 * b + e + 1) * nw])

    def swap(w, p):
        for b in (1, 0):
            d2d(w, p, b).start()

    def swapped(w, p):
        arrived(d2d_in.at[pl.ds(0, 2)], dr.at[w * pairs + p])

    def reduced(w, k):
        q = at(w, k)
        return part[q, core] + d2d_in[q]

    def push(w, k, to, group, value):
        rs_out[at(w, k)] = value.astype(jnp.bfloat16)
        send(w, k, to, group).start()

    def service(w, p):
        @pl.when((p >= 2) & (lax.rem(p, 2) == 1))
        def _():
            swapped(w, p)
            for b in (1, 0):
                k = member(p, b)
                push(w, k, 1, lax.div(p, 2), reduced(w, k))

        @pl.when(p == 1)
        def _():
            swapped(w, p)
            for k in (3, 1):
                push(w, k, k, 0, reduced(w, k))

    def service_far(w, p):
        @pl.when((p >= 2) & (lax.rem(p, 2) == 0))
        def _():
            swapped(w, p)
            arrived(blocks_of(2), rr.at[w, lax.div(p, 2)])
            for b in (1, 0):
                k = member(p, b)
                push(w, k, k, 0, reduced(w, k) + rs_in[at(w, k + 1)].astype(jnp.float32))

    def service_last(w):
        swapped(w, 0)
        push(w, 2, 2, 0, reduced(w, 2))
        own[w] = reduced(w, 0)

    evens = list(range(4, chips, 2))
    odds = [k + 1 for k in evens]

    def got(k):
        return 0 if k < 4 else 1 if k % 2 else k // 2

    def spread(w, k):
        return remote(ag.at[w, 0, core], ag.at[w, k, core], gs, gr.at[w, got(k)], peer(k))

    def relay(w, k):
        return remote(ag.at[w, k - 1, core], ag.at[w, k, core], gs, gr.at[w, got(k)], peer(1))

    def forward(w, k):
        return remote(ag.at[w, k, core], ag.at[w, k, core], fs, fr.at[w, k // 4 * 2 + k % 2], partner)

    def tell(k):
        return remote(lw.at[0], lw.at[k], ls, lr, peer(k))

    pair_sum = remote(lws.at[0], lws.at[1], ps, pr, partner)
    order = range(pairs)

    def combine(w):
        forces = own[w]
        arrived(blocks_of(3 + len(evens)), rr.at[w, 0])
        for k in evens + [1, 2, 3]:
            forces = forces + rs_in[at(w, k)].astype(jnp.float32)
        capped = jnp.tanh(forces)
        fields = nz[w] - capped
        ag[w, 0, core] = fields.astype(jnp.bfloat16)
        for k in evens[::-1] + [2, 3, 1] if w == waves - 1 else [2, 3, 1] + evens[::-1]:
            spread(w, k).start()
        forward(w, 0).start()
        row = jnp.sum(fields * capped - 0.5 * capped * capped, axis=0, keepdims=True)
        row = jnp.broadcast_to(row, lw.shape[1:])
        lw[0] = row if w == 0 else lw[0] + row
        if w == waves - 1:
            def start_tell(k, c):
                tell(k).start()
                return c

            lax.fori_loop(1, chips, start_tell, 0)

    def pull_near(w):
        arrived(blocks_of(3), gr.at[w, 0])
        for k in (1, 2, 3):
            forward(w, k).start()

    def pull_evens(w):
        for k in evens:
            arrived(blocks_of(1), gr.at[w, got(k)])
            relay(w, k + 1).start()
            forward(w, k).start()

    def pull_odds(w):
        if odds:
            arrived(blocks_of(len(odds)), gr.at[w, 1])
        for k in odds:
            forward(w, k).start()

    def settle(w, p):
        arrived(blocks_of(2), fr.at[w, p])

    def stage(w, p):
        blocks = []
        for b in range(2):
            for e in range(2):
                block = ag[w, member(p, b), e]
                for j in range(pack):
                    blocks.append(block[:, j * walkers:(j + 1) * walkers])
        lhs[...] = jnp.concatenate(blocks, axis=0).T
        value = jnp.dot(lhs[...], fac[pl.ds(base(w, p), deep), :], preferred_element_type=jnp.float32)
        pot[...] = value if w == 0 and p == order[0] else pot[...] + value

    green_in.wait()

    def step(t, c):
        w, p = where(t)
        product(w, p)

        @pl.when(t == 0)
        def _():
            pl.semaphore_wait(barrier, chips)

        swap(w, p)

        @pl.when(t > 1)
        def _():
            service_far(*where(t - 2))

        @pl.when(t > 0)
        def _():
            service(*where(t - 1))

        for v in range(waves - 1):
            @pl.when(t == (v + 1) * pairs)
            def _(v=v):
                service_last(v)

        @pl.when(t == 0)
        def _():
            noise_in.wait()
            turned = nzi[...].T
            for v in range(waves):
                nz[v] = pack_rows(turned[v * nw:(v + 1) * nw])

        for v in range(waves - 1):
            @pl.when(t == (v + 1) * pairs + pairs // 2)
            def _(v=v):
                combine(v)
        return c

    lax.fori_loop(0, steps, step, 0)
    def settle_weights():
        arrived(lw.at[pl.ds(1, chips - 1)], lr)
        acc = lw[0]
        for k in range(1, chips):
            acc = acc + lw[k]
        lws[0] = acc
        pair_sum.start()

    def write_weights():
        pair_sum.wait()
        packed = lws[0, 0:1, :] + lws[1, 0:1, :]
        row = packed[:, 0:walkers]
        for j in range(1, pack):
            row = row + packed[:, j * walkers:(j + 1) * walkers]
        per = walkers // n
        lane = lax.broadcasted_iota(jnp.int32, (1, walkers), 1)
        spot = lax.broadcasted_iota(jnp.int32, (8, 128), 1)
        mine = jnp.zeros((8, 128), jnp.float32)
        for j in range(per):
            one = jnp.sum(jnp.where(lane == me * per + j, row, 0.0), axis=1, keepdims=True)
            mine = jnp.where(spot == j, one, mine)
        logw[...] = mine / math.sqrt(total)

    if waves == 1:
        service_last(0)
        combine(0)
    for w in range(waves):
        last = w == waves - 1
        if last:
            pull_near(w)
            pull_evens(w)
        else:
            pull_near(w)
            service_last(w + 1)
            pull_evens(w)
        for i, p in enumerate(order):
            settle(w, p)
            stage(w, p)
            if not last and i == 0:
                combine(w + 1)
            if last and i == 0:
                settle_weights()
            if i == 1:
                pull_odds(w)
            if last and i == len(order) - 2:
                write_weights()

    arrived(d2d_in, ds)
    arrived(blocks_of(waves * (chips - 1)), rs)
    arrived(blocks_of(waves * (chips - 1)), gs)
    arrived(blocks_of(waves * chips), fs)
    arrived(lw.at[pl.ds(1, chips - 1)], ls)


def hand_over(pot, logw, pot_out, logw_out):
    pot_out[...] = pot[...]
    logw_out[...] = logw[0:1, 0:logw_out.shape[0]].reshape(logw_out.shape)


def solution(mesh):
    n = mesh.shape["chol"]

    def per_device(green, factors, noise):
        walkers, cols = green.shape
        total = factors.shape[0]
        chips = n // 2
        nv = total // n
        pack = max(1, 128 // walkers)
        waves = 2 if nv % (32 * pack) == 0 else 1
        half, lanes = nv // waves // pack, walkers * pack
        vmem = pl.BlockSpec(memory_space=pltpu.VMEM)
        hbm = pl.BlockSpec(memory_space=pltpu.HBM)
        dma = pltpu.SemaphoreType.DMA
        block = (waves * chips, half, lanes)
        pot, logw = pl.pallas_call(
            functools.partial(kernel, n, pack, waves),
            out_shape=(pltpu.VMEM((walkers, cols), jnp.float32), pltpu.VMEM((8, 128), jnp.float32)),
            in_specs=[hbm, hbm, hbm],
            out_specs=(vmem, vmem),
            scratch_shapes=[
                pltpu.VMEM(green.shape, jnp.bfloat16),
                pltpu.VMEM(noise.shape, jnp.float32),
                pltpu.VMEM(factors.shape, jnp.bfloat16),
                pltpu.VMEM((waves * chips, 2, half, lanes), jnp.float32),
                pltpu.VMEM(block, jnp.float32),
                pltpu.VMEM((waves, half, lanes), jnp.float32),
                pltpu.VMEM(block, jnp.bfloat16),
                pltpu.VMEM(block, jnp.bfloat16),
                pltpu.VMEM((waves, chips, 2, half, lanes), jnp.bfloat16),
                pltpu.VMEM((waves, half, lanes), jnp.float32),
                pltpu.VMEM((walkers, 4 * (nv // waves)), jnp.bfloat16),
                pltpu.VMEM((chips, 8, lanes), jnp.float32),
                pltpu.VMEM((2, 8, lanes), jnp.float32),
                dma((2,)), dma((waves * chips // 2,)),
                dma, dma((waves * chips // 2,)), dma, dma((waves, chips // 4)),
                dma, dma((waves, chips // 2)), dma, dma((waves, chips // 2)),
                dma, dma, dma, dma,
            ],
            compiler_params=pltpu.CompilerParams(
                collective_id=0, has_side_effects=True, vmem_limit_bytes=58 * 2**20),
        )(green, factors, noise)
        return pl.pallas_call(
            hand_over,
            out_shape=(jax.ShapeDtypeStruct((walkers, cols), jnp.float32),
                       jax.ShapeDtypeStruct((walkers // n,), jnp.float32)),
            in_specs=[vmem, vmem],
            out_specs=(vmem, vmem),
            compiler_params=pltpu.CompilerParams(vmem_limit_bytes=4 * 2**20),
        )(pot, logw)

    return jax.shard_map(
        per_device,
        mesh=mesh,
        in_specs=(P("groups", "chol"), P(None, "chol"), P("groups", "chol")),
        out_specs=(P("groups", "chol"), P(("groups", "chol"))),
        check_vma=False,
    )
```

```python
import functools
import math

import jax
import jax.numpy as jnp
from jax import lax
from jax.experimental import pallas as pl
from jax.experimental.pallas import tpu as pltpu
from jax.sharding import PartitionSpec as P

MESH = pl.DeviceIdType.MESH


def flip(a, b, bits):
    total = 0
    for bit in range(bits):
        x = lax.rem(lax.div(a, 2**bit), 2)
        y = lax.rem(lax.div(b, 2**bit), 2) if not isinstance(b, int) else (b >> bit) & 1
        total = total + (x + y - 2 * x * y) * 2**bit
    return total


def kernel(n, pack, waves, green, factors, noise, pot, logw,
           grn, nzi, fac, part, d2d_in, own, rs_out, rs_in, ag, nz, lhs, lw, lws,
           in_sem, fac_sem, ds, dr, rs, rr, gs, gr, fs, fr, ls, lr, ps, pr):
    chips = n // 2
    bits = chips.bit_length() - 1
    pairs = chips // 2
    total, cols = factors.shape
    nv = total // n
    nw = nv // waves
    half = nw // pack
    walkers = green.shape[0]
    deep = 4 * nw
    me = lax.axis_index("chol")
    chip, core = lax.div(me, 2), lax.rem(me, 2)
    other = 1 - core
    partner = chip * 2 + other

    def peer(k):
        return flip(chip, k, bits) * 2 + core

    def at(w, k):
        return w * chips + k

    def base(w, p):
        return pl.multiple_of((w * pairs + p) * deep, deep)

    def member(p, b):
        if isinstance(p, int):
            return p // 2 * 4 + p % 2 + 2 * b
        return lax.div(p, 2) * 4 + lax.rem(p, 2) + 2 * b

    def load(w, p, b, c):
        src = (flip(chip, member(p, b), bits) * 2 + c) * nv + w * nw
        return pltpu.make_async_copy(
            factors.at[pl.ds(pl.multiple_of(src, nw), nw), :],
            fac.at[pl.ds(pl.multiple_of(base(w, p) + (2 * b + c) * nw, nw), nw), :],
            fac_sem.at[w * pairs + p])

    green_in = pltpu.make_async_copy(green, grn, in_sem.at[0])
    noise_in = pltpu.make_async_copy(noise, nzi, in_sem.at[1])
    green_in.start()
    steps = waves * pairs

    def where(t):
        return lax.div(t, pairs), pairs - 1 - lax.rem(t, pairs)

    def start_load(t, c):
        w, p = where(t)
        for b in (0, 1):
            for e in range(2):
                load(w, p, b, e).start()
        return c

    noise_in.start()
    start_load(0, 0)
    lax.fori_loop(1, steps, start_load, 0)

    barrier = pltpu.get_barrier_semaphore()
    pl.semaphore_signal(barrier, inc=1, device_id={"chol": partner}, device_id_type=MESH)

    def greet(k, c):
        pl.semaphore_signal(barrier, inc=1, device_id={"chol": peer(k)}, device_id_type=MESH)
        return c

    lax.fori_loop(1, chips, greet, 0)

    def remote(src, dst, s, r, to):
        return pltpu.make_async_remote_copy(
            src_ref=src, dst_ref=dst, send_sem=s, recv_sem=r,
            device_id={"chol": to}, device_id_type=MESH)

    def arrived(ref, sem):
        pltpu.make_async_copy(ref, ref, sem).wait()

    def blocks_of(count):
        return rs_in.at[pl.ds(0, count)]

    def d2d(w, p, b):
        q = at(w, member(p, b))
        return remote(part.at[q, other], d2d_in.at[q], ds, dr.at[w * pairs + p], partner)

    def send(w, k, to, group):
        q = at(w, k)
        return remote(rs_out.at[q], rs_in.at[q], rs, rr.at[w, group], peer(to))

    def pack_rows(o):
        rows = [o[j * half:(j + 1) * half] for j in range(pack)]
        return jnp.concatenate(rows, axis=1) if pack > 1 else rows[0]

    def product(w, p):
        arrived(fac.at[pl.ds(base(w, p), deep), :], fac_sem.at[w * pairs + p])
        o = lax.dot_general(fac[pl.ds(base(w, p), deep), :], grn[...], (((1,), (1,)), ((), ())),
                            preferred_element_type=jnp.float32)
        for b in range(2):
            for e in range(2):
                part[at(w, member(p, b)), e] = pack_rows(o[(2 * b + e) * nw:(2 * b + e + 1) * nw])

    def swap(w, p):
        for b in (1, 0):
            d2d(w, p, b).start()

    def swapped(w, p):
        arrived(d2d_in.at[pl.ds(0, 2)], dr.at[w * pairs + p])

    def reduced(w, k):
        q = at(w, k)
        return part[q, core] + d2d_in[q]

    def push(w, k, to, group, value):
        rs_out[at(w, k)] = value.astype(jnp.bfloat16)
        send(w, k, to, group).start()

    def service(w, p):
        @pl.when((p >= 2) & (lax.rem(p, 2) == 1))
        def _():
            swapped(w, p)
            for b in (1, 0):
                k = member(p, b)
                push(w, k, 1, lax.div(p, 2), reduced(w, k))

        @pl.when(p == 1)
        def _():
            swapped(w, p)
            for k in (3, 1):
                push(w, k, k, 0, reduced(w, k))

    def service_far(w, p):
        @pl.when((p >= 2) & (lax.rem(p, 2) == 0))
        def _():
            swapped(w, p)
            arrived(blocks_of(2), rr.at[w, lax.div(p, 2)])
            for b in (1, 0):
                k = member(p, b)
                push(w, k, k, 0, reduced(w, k) + rs_in[at(w, k + 1)].astype(jnp.float32))

    def service_last(w):
        swapped(w, 0)
        push(w, 2, 2, 0, reduced(w, 2))
        own[w] = reduced(w, 0)

    evens = list(range(4, chips, 2))
    odds = [k + 1 for k in evens]

    def got(k):
        return 0 if k < 4 else 1 if k % 2 else k // 2

    def spread(w, k):
        return remote(ag.at[w, 0, core], ag.at[w, k, core], gs, gr.at[w, got(k)], peer(k))

    def relay(w, k):
        return remote(ag.at[w, k - 1, core], ag.at[w, k, core], gs, gr.at[w, got(k)], peer(1))

    def forward(w, k):
        return remote(ag.at[w, k, core], ag.at[w, k, core], fs, fr.at[w, k // 4 * 2 + k % 2], partner)

    def tell(k):
        return remote(lw.at[0], lw.at[k], ls, lr, peer(k))

    pair_sum = remote(lws.at[0], lws.at[1], ps, pr, partner)
    order = range(pairs)

    def combine(w):
        forces = own[w]
        arrived(blocks_of(3 + len(evens)), rr.at[w, 0])
        for k in evens + [1, 2, 3]:
            forces = forces + rs_in[at(w, k)].astype(jnp.float32)
        capped = jnp.tanh(forces)
        fields = nz[w] - capped
        ag[w, 0, core] = fields.astype(jnp.bfloat16)
        for k in evens[::-1] + [2, 3, 1] if w == waves - 1 else [2, 3, 1] + evens[::-1]:
            spread(w, k).start()
        forward(w, 0).start()
        row = jnp.sum(fields * capped - 0.5 * capped * capped, axis=0, keepdims=True)
        row = jnp.broadcast_to(row, lw.shape[1:])
        lw[0] = row if w == 0 else lw[0] + row
        if w == waves - 1:
            def start_tell(k, c):
                tell(k).start()
                return c

            lax.fori_loop(1, chips, start_tell, 0)

    def pull_near(w):
        arrived(blocks_of(3), gr.at[w, 0])
        for k in (1, 2, 3):
            forward(w, k).start()

    def pull_evens(w):
        for k in evens:
            arrived(blocks_of(1), gr.at[w, got(k)])
            relay(w, k + 1).start()
            forward(w, k).start()

    def pull_odds(w):
        if odds:
            arrived(blocks_of(len(odds)), gr.at[w, 1])
        for k in odds:
            forward(w, k).start()

    def settle(w, p):
        arrived(blocks_of(2), fr.at[w, p])

    def stage(w, p):
        blocks = []
        for b in range(2):
            for e in range(2):
                block = ag[w, member(p, b), e]
                for j in range(pack):
                    blocks.append(block[:, j * walkers:(j + 1) * walkers])
        lhs[...] = jnp.concatenate(blocks, axis=0).T
        value = jnp.dot(lhs[...], fac[pl.ds(base(w, p), deep), :], preferred_element_type=jnp.float32)
        pot[...] = value if w == 0 and p == order[0] else pot[...] + value

    noise_in.wait()
    turned = nzi[...].T
    for v in range(waves):
        nz[v] = pack_rows(turned[v * nw:(v + 1) * nw])
    green_in.wait()

    def step(t, c):
        w, p = where(t)
        product(w, p)

        @pl.when(t == 0)
        def _():
            pl.semaphore_wait(barrier, chips)

        swap(w, p)

        @pl.when(t > 1)
        def _():
            service_far(*where(t - 2))

        @pl.when(t > 0)
        def _():
            service(*where(t - 1))

        for v in range(waves - 1):
            @pl.when(t == (v + 1) * pairs)
            def _(v=v):
                service_last(v)

        for v in range(waves - 1):
            @pl.when(t == (v + 1) * pairs + pairs // 2)
            def _(v=v):
                combine(v)
        return c

    lax.fori_loop(0, steps, step, 0)
    def settle_weights():
        arrived(lw.at[pl.ds(1, chips - 1)], lr)
        acc = lw[0]
        for k in range(1, chips):
            acc = acc + lw[k]
        lws[0] = acc
        pair_sum.start()

    def write_weights():
        pair_sum.wait()
        packed = lws[0, 0:1, :] + lws[1, 0:1, :]
        row = packed[:, 0:walkers]
        for j in range(1, pack):
            row = row + packed[:, j * walkers:(j + 1) * walkers]
        per = walkers // n
        lane = lax.broadcasted_iota(jnp.int32, (1, walkers), 1)
        spot = lax.broadcasted_iota(jnp.int32, (8, 128), 1)
        mine = jnp.zeros((8, 128), jnp.float32)
        for j in range(per):
            one = jnp.sum(jnp.where(lane == me * per + j, row, 0.0), axis=1, keepdims=True)
            mine = jnp.where(spot == j, one, mine)
        logw[...] = mine / math.sqrt(total)

    if waves == 1:
        service_last(0)
        combine(0)
    for w in range(waves):
        last = w == waves - 1
        if last:
            pull_near(w)
            pull_evens(w)
        else:
            pull_near(w)
            service_last(w + 1)
            pull_evens(w)
        for i, p in enumerate(order):
            settle(w, p)
            stage(w, p)
            if not last and i == 0:
                combine(w + 1)
            if last and i == 0:
                settle_weights()
            if i == 1:
                pull_odds(w)
            if last and i == len(order) - 2:
                write_weights()

    arrived(d2d_in, ds)
    arrived(blocks_of(waves * (chips - 1)), rs)
    arrived(blocks_of(waves * (chips - 1)), gs)
    arrived(blocks_of(waves * chips), fs)
    arrived(lw.at[pl.ds(1, chips - 1)], ls)


def hand_over(pot, logw, pot_out, logw_out):
    pot_out[...] = pot[...]
    logw_out[...] = logw[0:1, 0:logw_out.shape[0]].reshape(logw_out.shape)


def solution(mesh):
    n = mesh.shape["chol"]

    def per_device(green, factors, noise):
        walkers, cols = green.shape
        total = factors.shape[0]
        chips = n // 2
        nv = total // n
        pack = max(1, 128 // walkers)
        waves = 2 if nv % (32 * pack) == 0 else 1
        half, lanes = nv // waves // pack, walkers * pack
        vmem = pl.BlockSpec(memory_space=pltpu.VMEM)
        hbm = pl.BlockSpec(memory_space=pltpu.HBM)
        dma = pltpu.SemaphoreType.DMA
        block = (waves * chips, half, lanes)
        pot, logw = pl.pallas_call(
            functools.partial(kernel, n, pack, waves),
            out_shape=(pltpu.VMEM((walkers, cols), jnp.float32), pltpu.VMEM((8, 128), jnp.float32)),
            in_specs=[hbm, hbm, hbm],
            out_specs=(vmem, vmem),
            scratch_shapes=[
                pltpu.VMEM(green.shape, jnp.bfloat16),
                pltpu.VMEM(noise.shape, jnp.float32),
                pltpu.VMEM(factors.shape, jnp.bfloat16),
                pltpu.VMEM((waves * chips, 2, half, lanes), jnp.float32),
                pltpu.VMEM(block, jnp.float32),
                pltpu.VMEM((waves, half, lanes), jnp.float32),
                pltpu.VMEM(block, jnp.bfloat16),
                pltpu.VMEM(block, jnp.bfloat16),
                pltpu.VMEM((waves, chips, 2, half, lanes), jnp.bfloat16),
                pltpu.VMEM((waves, half, lanes), jnp.float32),
                pltpu.VMEM((walkers, 4 * (nv // waves)), jnp.bfloat16),
                pltpu.VMEM((chips, 8, lanes), jnp.float32),
                pltpu.VMEM((2, 8, lanes), jnp.float32),
                dma((2,)), dma((waves * chips // 2,)),
                dma, dma((waves * chips // 2,)), dma, dma((waves, chips // 4)),
                dma, dma((waves, chips // 2)), dma, dma((waves, chips // 2)),
                dma, dma, dma, dma,
            ],
            compiler_params=pltpu.CompilerParams(
                collective_id=0, has_side_effects=True, vmem_limit_bytes=58 * 2**20),
        )(green, factors, noise)
        return pl.pallas_call(
            hand_over,
            out_shape=(jax.ShapeDtypeStruct((walkers, cols), jnp.float32),
                       jax.ShapeDtypeStruct((walkers // n,), jnp.float32)),
            in_specs=[vmem, vmem],
            out_specs=(vmem, vmem),
            compiler_params=pltpu.CompilerParams(vmem_limit_bytes=4 * 2**20),
        )(pot, logw)

    return jax.shard_map(
        per_device,
        mesh=mesh,
        in_specs=(P("groups", "chol"), P(None, "chol"), P("groups", "chol")),
        out_specs=(P("groups", "chol"), P(("groups", "chol"))),
        check_vma=False,
    )
```
